32 devices in a mesh: owner: 8 (over y, x, core), rows: 4 (over z).
Axes of the slice: x: 2, y: 2, z: 4, core: 2. Of those that a mesh axis runs over, the one named last changes fastest.
Arguments:
- w_down: float32 [64, 1024, 2048], P('owner', None, 'rows'), may hold values from -0.1875 to 0.1875
- router_weight: float32 [2048, 64], P('rows', 'owner'), may hold values from -0.125 to 0.125
- router_gain: float32 [2048], P('rows'), may hold values from 0.25 to 1.75
Outputs:
- serve_down: bfloat16 [64, 2048, 1024], P('owner')
- serve_router: bfloat16 [2048, 64], replicated
The draws below stay inside these ranges and needn't reach their ends.
All inputs are finite; a program needn't handle non-finite values.
Results may differ from the reference program's by a relative error of at most 0.001.
Values may be sent and summed in bfloat16 or wider, within the bound.
A program may use at most 128 MiB of HBM per device.

```python
import jax
import jax.numpy as jnp

EXPERTS = 64
D_MODEL = 2048
D_EXPERT = 1024


def block_scale(rng, dims, pieces, low, top_value):
    def one(dim, shards_of):
        draws = jax.random.uniform(jax.random.fold_in(jax.random.fold_in(rng, 6), dim), (shards_of,), jnp.float32, low / len(pieces), top_value / len(pieces))
        return jnp.repeat(jnp.exp(draws), dims[dim] // shards_of).reshape((-1,) + (1,) * (len(dims) - dim - 1))

    factor_of = one(*pieces[0])
    for cut in pieces[1:]:
        factor_of = factor_of * one(*cut)
    return factor_of


def noise(stream_key, extent, spread, bound, pieces=(), held_as=jnp.bfloat16):
    drawn = jax.random.normal(stream_key, extent, jnp.float32) * spread
    if len(pieces) > 0:
        drawn = block_scale(stream_key, extent, pieces, -0.22, 0.18) * drawn
    return jnp.clip(drawn, min=-bound, max=bound).astype(held_as)


def setup_inputs(seed: int = 0) -> dict:
    splits = jax.random.split(jax.random.key(seed), 4)
    return {
        "w_down": noise(splits[0], (EXPERTS, D_EXPERT, D_MODEL), D_EXPERT ** -0.5, 0.1875, ((0, 8), (2, 4)), jnp.float32),
        "router_weight": noise(splits[1], (D_MODEL, EXPERTS), D_MODEL ** -0.5, 0.125, ((0, 4), (1, 8)), jnp.float32),
        "router_gain": jnp.clip(1.0 + 0.15 * jax.random.normal(splits[2], (D_MODEL,), jnp.float32), 0.25, 1.75),
    }


def reference(w_down, router_weight, router_gain):
    serve_down = w_down.astype(jnp.bfloat16)
    serve_down = jnp.transpose(serve_down, (0, 2, 1))
    serve_router = (router_weight * router_gain[:, None]).astype(jnp.bfloat16)
    return serve_down, serve_router
```

```python
import functools

import jax
import jax.numpy as jnp
from jax import lax
from jax.experimental import pallas as pl
from jax.experimental.pallas import tpu as pltpu
from jax.sharding import PartitionSpec as P

MESH = pl.DeviceIdType.MESH
TAIL = 1


def gather_kernel(n, owners, tail, w_ref, part_ref, down_ref, router_ref, wide, own, load_sem, local_sem,
                  send_sem, recv_sem, router_local, rows_send, rows_recv, owner_send, owner_recv):
    me = lax.axis_index("rows")
    mine = lax.axis_index("owner")
    experts, depth, width = w_ref.shape
    last = n - 1

    def rows_of(block):
        return pl.ds(pl.multiple_of(block * width, width), width)

    barrier = pltpu.get_barrier_semaphore()

    @pl.loop(1, n)
    def _(d):
        pl.semaphore_signal(barrier, inc=1, device_id={"rows": lax.rem(me + d, n)}, device_id_type=MESH)

    @pl.loop(1, owners)
    def _(d):
        pl.semaphore_signal(barrier, inc=1, device_id={"owner": lax.rem(mine + d, owners)}, device_id_type=MESH)

    def load(e, slot):
        return pltpu.make_async_copy(w_ref.at[e], wide.at[slot], load_sem.at[slot])

    def keep(e):
        return pltpu.make_async_copy(own.at[e], down_ref.at[e, rows_of(me), :], local_sem.at[e])

    def send(src, way, hop, e, block):
        peer = me + 1 if way == 0 else me - 1
        return pltpu.make_async_remote_copy(
            src_ref=src, dst_ref=down_ref.at[e, rows_of(block), :],
            send_sem=send_sem.at[way, hop, e], recv_sem=recv_sem.at[way, hop, e],
            device_id={"rows": peer}, device_id_type=MESH)

    def rows_copy(peer):
        return pltpu.make_async_remote_copy(
            src_ref=part_ref, dst_ref=router_ref.at[mine, me],
            send_sem=rows_send.at[peer], recv_sem=rows_recv.at[me],
            device_id={"rows": peer}, device_id_type=MESH)

    def rows_arrival(peer):
        return pltpu.make_async_remote_copy(
            src_ref=part_ref, dst_ref=router_ref.at[mine, peer],
            send_sem=rows_send.at[peer], recv_sem=rows_recv.at[peer],
            device_id={"rows": peer}, device_id_type=MESH)

    def owner_copy(peer):
        return pltpu.make_async_remote_copy(
            src_ref=router_ref.at[mine], dst_ref=router_ref.at[mine],
            send_sem=owner_send.at[peer], recv_sem=owner_recv.at[mine],
            device_id={"owner": peer}, device_id_type=MESH)

    def owner_arrival(peer):
        return pltpu.make_async_remote_copy(
            src_ref=router_ref.at[mine], dst_ref=router_ref.at[peer],
            send_sem=owner_send.at[peer], recv_sem=owner_recv.at[peer],
            device_id={"owner": peer}, device_id_type=MESH)

    load(0, 0).start()
    own_part = pltpu.make_async_copy(part_ref, router_ref.at[mine, me], router_local)
    own_part.start()

    @pl.loop(0, experts)
    def _(e):
        slot = lax.rem(e, 2)

        @pl.when(e + 1 < experts)
        def _():
            load(e + 1, 1 - slot).start()

        load(e, slot).wait()
        own[e] = wide[slot].astype(jnp.bfloat16).T

        @pl.when(e == 0)
        def _():
            pl.semaphore_wait(barrier, n - 1 + owners - 1)

            @pl.loop(1, n)
            def _(d):
                rows_copy(lax.rem(me + d, n)).start()

        @pl.when(me < last)
        def _():
            send(own.at[e], 0, 0, e, me).start()

        @pl.when(me > 0)
        def _():
            send(own.at[e], 1, 0, e, me).start()

        keep(e).start()

    own_part.wait()

    @pl.loop(1, n)
    def _(d):
        rows_arrival(lax.rem(me + d, n)).wait_recv()

    @pl.loop(1, owners)
    def _(d):
        owner_copy(lax.rem(mine + d, owners)).start()

    def pass_on(k):
        hop = k // experts
        e = lax.rem(k, experts)
        ahead = me - 1 - hop
        behind = me + 1 + hop

        @pl.when(ahead >= 0)
        def _():
            block = down_ref.at[e, rows_of(ahead), :]
            send(block, 0, hop, e, ahead).wait_recv()
            on = (me < last) & ((hop + 2 < last) | (e < experts - tail))

            @pl.when(on)
            def _():
                send(block, 0, hop + 1, e, ahead).start()

        @pl.when(behind < n)
        def _():
            block = down_ref.at[e, rows_of(behind), :]
            send(block, 1, hop, e, behind).wait_recv()
            on = (me > 0) & ((hop + 2 < last) | (e < experts - tail))

            @pl.when(on)
            def _():
                send(block, 1, hop + 1, e, behind).start()

    @pl.loop(0, last * experts - tail)
    def _(k):
        pass_on(k)

    @pl.loop(0, experts)
    def _(e):
        keep(e).wait()

    @pl.loop(0, last * experts - tail)
    def _(k):
        hop = k // experts
        e = lax.rem(k, experts)
        ahead = me - hop
        behind = me + hop

        @pl.when((ahead >= 0) & (me < last))
        def _():
            send(own.at[e], 0, hop, e, me).wait_send()

        @pl.when((behind < n) & (me > 0))
        def _():
            send(own.at[e], 1, hop, e, me).wait_send()

    @pl.loop(1, n)
    def _(d):
        rows_copy(lax.rem(me + d, n)).wait_send()

    @pl.loop(1, owners)
    def _(d):
        owner_arrival(lax.rem(mine + d, owners)).wait_recv()
        owner_copy(lax.rem(mine + d, owners)).wait_send()


def copy_kernel(src_ref, dst_ref):
    dst_ref[...] = src_ref[...]


def place_kernel(n, tail, down_ref, piece_ref, out_ref, sem):
    me = lax.axis_index("rows")
    experts = out_ref.shape[0]
    width = piece_ref.shape[1]

    def place(block):
        return pltpu.make_async_copy(
            piece_ref, out_ref.at[pl.ds(experts - tail, tail), pl.ds(block * width, width), :], sem)

    @pl.when(me == 0)
    def _():
        place(n - 1).start()
        place(n - 1).wait()

    @pl.when(me == n - 1)
    def _():
        place(0).start()
        place(0).wait()


def shards(n, owners, w_down, router_weight, router_gain):
    experts, depth, width = w_down.shape
    tail = TAIL if n > 2 else 0
    part = (router_weight * router_gain[:, None]).astype(jnp.bfloat16).T
    cols, rows = part.shape
    hbm = pl.BlockSpec(memory_space=pl.ANY)
    vmem = pl.BlockSpec(memory_space=pltpu.VMEM)
    down, router = pl.pallas_call(
        functools.partial(gather_kernel, n, owners, tail),
        out_shape=(jax.ShapeDtypeStruct((experts, n * width, depth), jnp.bfloat16),
                   jax.ShapeDtypeStruct((owners, n, cols, rows), jnp.bfloat16)),
        in_specs=[hbm, vmem],
        out_specs=(hbm, vmem),
        scratch_shapes=[
            pltpu.VMEM((2, depth, width), jnp.float32),
            pltpu.VMEM((experts, width, depth), jnp.bfloat16),
            pltpu.SemaphoreType.DMA((2,)),
            pltpu.SemaphoreType.DMA((experts,)),
            pltpu.SemaphoreType.DMA((2, n - 1, experts)),
            pltpu.SemaphoreType.DMA((2, n - 1, experts)),
            pltpu.SemaphoreType.DMA,
            pltpu.SemaphoreType.DMA((n,)),
            pltpu.SemaphoreType.DMA((n,)),
            pltpu.SemaphoreType.DMA((owners,)),
            pltpu.SemaphoreType.DMA((owners,)),
        ],
        compiler_params=pltpu.CompilerParams(collective_id=0, has_side_effects=True,
                                             vmem_limit_bytes=40 * 1024 * 1024),
    )(w_down, part)
    serve_router = router.transpose(1, 3, 0, 2).reshape(n * rows, owners * cols)
    if tail == 0:
        return down, serve_router
    me = lax.axis_index("rows")
    start = jnp.where(me == n - 2, 0, (n - 1) * width)
    piece = lax.dynamic_slice(down, (experts - tail, start, 0), (tail, width, depth))
    piece = lax.ppermute(piece, "rows", [(n - 2, n - 1), (1, 0)])
    block = (1, n * width // 2, depth)
    out = pl.pallas_call(
        copy_kernel,
        out_shape=jax.ShapeDtypeStruct(down.shape, down.dtype),
        grid=(experts, 2),
        in_specs=[pl.BlockSpec(block, lambda e, h: (e, h, 0))],
        out_specs=pl.BlockSpec(block, lambda e, h: (e, h, 0)),
        cost_estimate=pl.CostEstimate(flops=0, transcendentals=0, bytes_accessed=4 * down.size),
    )(down)
    out = pl.pallas_call(
        functools.partial(place_kernel, n, tail),
        out_shape=jax.ShapeDtypeStruct(down.shape, down.dtype),
        in_specs=[hbm, vmem],
        out_specs=hbm,
        scratch_shapes=[pltpu.SemaphoreType.DMA],
        input_output_aliases={0: 0},
    )(out, piece)
    return out, serve_router


def solution(mesh):
    n, owners = mesh.shape["rows"], mesh.shape["owner"]
    in_specs = (P("owner", None, "rows"), P("rows", "owner"), P("rows"))
    out_specs = (P("owner", None, None), P())
    return jax.shard_map(functools.partial(shards, n, owners), mesh=mesh, in_specs=in_specs,
                         out_specs=out_specs, check_vma=False)
```

```python
import functools

import jax
import jax.numpy as jnp
from jax import lax
from jax.experimental import pallas as pl
from jax.experimental.pallas import tpu as pltpu
from jax.sharding import PartitionSpec as P

MESH = pl.DeviceIdType.MESH
TAIL = 2


def gather_kernel(n, owners, tail, w_ref, part_ref, down_ref, router_ref, wide, own, load_sem, local_sem,
                  send_sem, recv_sem, router_local, rows_send, rows_recv, owner_send, owner_recv):
    me = lax.axis_index("rows")
    mine = lax.axis_index("owner")
    experts, depth, width = w_ref.shape
    last = n - 1

    def rows_of(block):
        return pl.ds(pl.multiple_of(block * width, width), width)

    barrier = pltpu.get_barrier_semaphore()

    @pl.loop(1, n)
    def _(d):
        pl.semaphore_signal(barrier, inc=1, device_id={"rows": lax.rem(me + d, n)}, device_id_type=MESH)

    @pl.loop(1, owners)
    def _(d):
        pl.semaphore_signal(barrier, inc=1, device_id={"owner": lax.rem(mine + d, owners)}, device_id_type=MESH)

    def load(e, slot):
        return pltpu.make_async_copy(w_ref.at[e], wide.at[slot], load_sem.at[slot])

    def keep(e):
        return pltpu.make_async_copy(own.at[e], down_ref.at[e, rows_of(me), :], local_sem.at[e])

    def send(src, way, hop, e, block):
        peer = me + 1 if way == 0 else me - 1
        return pltpu.make_async_remote_copy(
            src_ref=src, dst_ref=down_ref.at[e, rows_of(block), :],
            send_sem=send_sem.at[way, hop, e], recv_sem=recv_sem.at[way, hop, e],
            device_id={"rows": peer}, device_id_type=MESH)

    def rows_copy(peer):
        return pltpu.make_async_remote_copy(
            src_ref=part_ref, dst_ref=router_ref.at[mine, me],
            send_sem=rows_send.at[peer], recv_sem=rows_recv.at[me],
            device_id={"rows": peer}, device_id_type=MESH)

    def rows_arrival(peer):
        return pltpu.make_async_remote_copy(
            src_ref=part_ref, dst_ref=router_ref.at[mine, peer],
            send_sem=rows_send.at[peer], recv_sem=rows_recv.at[peer],
            device_id={"rows": peer}, device_id_type=MESH)

    def owner_copy(peer):
        return pltpu.make_async_remote_copy(
            src_ref=router_ref.at[mine], dst_ref=router_ref.at[mine],
            send_sem=owner_send.at[peer], recv_sem=owner_recv.at[mine],
            device_id={"owner": peer}, device_id_type=MESH)

    def owner_arrival(peer):
        return pltpu.make_async_remote_copy(
            src_ref=router_ref.at[mine], dst_ref=router_ref.at[peer],
            send_sem=owner_send.at[peer], recv_sem=owner_recv.at[peer],
            device_id={"owner": peer}, device_id_type=MESH)

    load(0, 0).start()
    own_part = pltpu.make_async_copy(part_ref, router_ref.at[mine, me], router_local)
    own_part.start()

    @pl.loop(0, experts)
    def _(e):
        slot = lax.rem(e, 2)

        @pl.when(e + 1 < experts)
        def _():
            load(e + 1, 1 - slot).start()

        load(e, slot).wait()
        own[e] = wide[slot].astype(jnp.bfloat16).T

        @pl.when(e == 0)
        def _():
            pl.semaphore_wait(barrier, n - 1 + owners - 1)

            @pl.loop(1, n)
            def _(d):
                rows_copy(lax.rem(me + d, n)).start()

        @pl.when(me < last)
        def _():
            send(own.at[e], 0, 0, e, me).start()

        @pl.when(me > 0)
        def _():
            send(own.at[e], 1, 0, e, me).start()

        keep(e).start()

    own_part.wait()

    @pl.loop(1, n)
    def _(d):
        rows_arrival(lax.rem(me + d, n)).wait_recv()

    @pl.loop(1, owners)
    def _(d):
        owner_copy(lax.rem(mine + d, owners)).start()

    def pass_on(k):
        hop = k // experts
        e = lax.rem(k, experts)
        ahead = me - 1 - hop
        behind = me + 1 + hop

        @pl.when(ahead >= 0)
        def _():
            block = down_ref.at[e, rows_of(ahead), :]
            send(block, 0, hop, e, ahead).wait_recv()
            on = (me < last) & ((hop + 2 < last) | (e < experts - tail))

            @pl.when(on)
            def _():
                send(block, 0, hop + 1, e, ahead).start()

        @pl.when(behind < n)
        def _():
            block = down_ref.at[e, rows_of(behind), :]
            send(block, 1, hop, e, behind).wait_recv()
            on = (me > 0) & ((hop + 2 < last) | (e < experts - tail))

            @pl.when(on)
            def _():
                send(block, 1, hop + 1, e, behind).start()

    @pl.loop(0, last * experts - tail)
    def _(k):
        pass_on(k)

    @pl.loop(0, experts)
    def _(e):
        keep(e).wait()

    @pl.loop(0, last * experts - tail)
    def _(k):
        hop = k // experts
        e = lax.rem(k, experts)
        ahead = me - hop
        behind = me + hop

        @pl.when((ahead >= 0) & (me < last))
        def _():
            send(own.at[e], 0, hop, e, me).wait_send()

        @pl.when((behind < n) & (me > 0))
        def _():
            send(own.at[e], 1, hop, e, me).wait_send()

    @pl.loop(1, n)
    def _(d):
        rows_copy(lax.rem(me + d, n)).wait_send()

    @pl.loop(1, owners)
    def _(d):
        owner_arrival(lax.rem(mine + d, owners)).wait_recv()
        owner_copy(lax.rem(mine + d, owners)).wait_send()


def copy_kernel(src_ref, dst_ref):
    dst_ref[...] = src_ref[...]


def place_kernel(n, expert, down_ref, piece_ref, out_ref, sem):
    me = lax.axis_index("rows")
    width = piece_ref.shape[1]

    def place(block):
        return pltpu.make_async_copy(
            piece_ref, out_ref.at[pl.ds(expert, 1), pl.ds(block * width, width), :], sem)

    @pl.when(me == 0)
    def _():
        place(n - 1).start()
        place(n - 1).wait()

    @pl.when(me == n - 1)
    def _():
        place(0).start()
        place(0).wait()


def shards(n, owners, w_down, router_weight, router_gain):
    experts, depth, width = w_down.shape
    tail = min(TAIL, experts) if n > 3 else 0
    part = (router_weight * router_gain[:, None]).astype(jnp.bfloat16).T
    cols, rows = part.shape
    hbm = pl.BlockSpec(memory_space=pl.ANY)
    vmem = pl.BlockSpec(memory_space=pltpu.VMEM)
    down, router = pl.pallas_call(
        functools.partial(gather_kernel, n, owners, tail),
        out_shape=(jax.ShapeDtypeStruct((experts, n * width, depth), jnp.bfloat16),
                   jax.ShapeDtypeStruct((owners, n, cols, rows), jnp.bfloat16)),
        in_specs=[hbm, vmem],
        out_specs=(hbm, vmem),
        scratch_shapes=[
            pltpu.VMEM((2, depth, width), jnp.float32),
            pltpu.VMEM((experts, width, depth), jnp.bfloat16),
            pltpu.SemaphoreType.DMA((2,)),
            pltpu.SemaphoreType.DMA((experts,)),
            pltpu.SemaphoreType.DMA((2, n - 1, experts)),
            pltpu.SemaphoreType.DMA((2, n - 1, experts)),
            pltpu.SemaphoreType.DMA,
            pltpu.SemaphoreType.DMA((n,)),
            pltpu.SemaphoreType.DMA((n,)),
            pltpu.SemaphoreType.DMA((owners,)),
            pltpu.SemaphoreType.DMA((owners,)),
        ],
        compiler_params=pltpu.CompilerParams(collective_id=0, has_side_effects=True,
                                             vmem_limit_bytes=40 * 1024 * 1024),
    )(w_down, part)
    serve_router = router.transpose(1, 3, 0, 2).reshape(n * rows, owners * cols)
    if tail == 0:
        return down, serve_router
    me = lax.axis_index("rows")
    start = jnp.where(me == n - 2, 0, (n - 1) * width)
    late = range(experts - tail, experts)
    pieces = []
    for e in late:
        piece = lax.dynamic_slice(down, (e, start, 0), (1, width, depth))
        pieces.append(lax.ppermute(piece, "rows", [(n - 2, n - 1), (1, 0)]))
    block = (1, n * width // 2, depth)
    out = pl.pallas_call(
        copy_kernel,
        out_shape=jax.ShapeDtypeStruct(down.shape, down.dtype),
        grid=(experts, 2),
        in_specs=[pl.BlockSpec(block, lambda e, h: (e, h, 0))],
        out_specs=pl.BlockSpec(block, lambda e, h: (e, h, 0)),
        compiler_params=pltpu.CompilerParams(vmem_limit_bytes=24 * 1024 * 1024),
        cost_estimate=pl.CostEstimate(flops=0, transcendentals=0, bytes_accessed=4 * down.size),
    )(down)
    for e, piece in zip(late, pieces):
        out = pl.pallas_call(
            functools.partial(place_kernel, n, e),
            out_shape=jax.ShapeDtypeStruct(down.shape, down.dtype),
            in_specs=[hbm, vmem],
            out_specs=hbm,
            scratch_shapes=[pltpu.SemaphoreType.DMA],
            input_output_aliases={0: 0},
            compiler_params=pltpu.CompilerParams(vmem_limit_bytes=8 * 1024 * 1024),
            cost_estimate=pl.CostEstimate(flops=0, transcendentals=0, bytes_accessed=4 * piece.size),
        )(out, piece)
    return out, serve_router


def solution(mesh):
    n, owners = mesh.shape["rows"], mesh.shape["owner"]
    in_specs = (P("owner", None, "rows"), P("rows", "owner"), P("rows"))
    out_specs = (P("owner", None, None), P())
    return jax.shard_map(functools.partial(shards, n, owners), mesh=mesh, in_specs=in_specs,
                         out_specs=out_specs, check_vma=False)
```
